32 devices in a mesh: row: 8 (over z, y), col: 4 (over x, core).
Axes of the slice: x: 2, y: 2, z: 4, core: 2. Of those that a mesh axis runs over, the one named last changes fastest.
Arguments:
- embeddings: bfloat16 [12288, 768], P(('row', 'col'))
- doc_order: int32 [12288], P(('row', 'col')), may hold values from 0 to 12287, each once
Outputs:
- nearest_earlier: float32 [12288], P(('row', 'col'))
The draws below stay inside these ranges and needn't reach their ends.
Inputs may be any that keep to these rules, and one draw needn't show every extreme that they name: `doc_order`: each value 0 to 12287 appears once.
All inputs are finite; a program needn't handle non-finite values.
Results may differ from the reference program's by a relative error of at most 0.00051.
Values may be sent and summed in bfloat16 or wider, within the bound.
A program may use at most 64 MiB of HBM per device.

```python
import jax
import jax.numpy as jnp
from jax import lax

D = 768
N = 12288


def draw_embeddings(key, part):
    groups = max(N // 4, 1)
    key_group = jax.random.fold_in(key, 11)
    key_amp = jax.random.fold_in(key, 12)
    key_center = jax.random.fold_in(key, 13)
    key_noise = jax.random.fold_in(key, 14)
    member = jax.random.randint(key_group, (N,), 0, groups)
    amplitude = jax.random.uniform(key_amp, (groups,), jnp.float32, 0.5, 3.0)
    centers = jax.random.normal(key_center, (groups, D), jnp.float32)
    noise = jax.random.normal(key_noise, (N, D), jnp.float32)
    values = noise + amplitude[member][:, None] * centers[member]
    return values.astype(jnp.bfloat16)


def setup_inputs(seed: int = 0) -> dict:
    streams_of = jax.random.split(jax.random.key(seed), 3)
    embeddings = draw_embeddings(jax.random.fold_in(streams_of[2], 71), 0)
    doc_order = jax.random.permutation(streams_of[1], N).astype(jnp.int32)
    return dict(embeddings=embeddings, doc_order=doc_order)


def normalize_rows(embeddings):
    floats = embeddings.astype(jnp.float32)
    scale = lax.rsqrt(lax.optimization_barrier(jnp.sum(floats * floats, axis=1, keepdims=True)) + 1e-06)
    return (floats * scale).astype(jnp.bfloat16)

def reference(embeddings, doc_order):
    unit_rows = normalize_rows(embeddings)
    block_rows = 1024 if N % 1024 == 0 else N
    row_groups = unit_rows.reshape(N // block_rows, block_rows, D)
    order_groups = doc_order.reshape(N // block_rows, block_rows)

    def one_block(pair):
        rows_here, orders_here = pair
        scores = jnp.dot(rows_here, unit_rows.T, preferred_element_type=jnp.float32)
        earlier = doc_order[None, :] < orders_here[:, None]
        masked = jnp.where(earlier, scores, jnp.float32(-1.0))
        return jnp.maximum(lax.optimization_barrier(jnp.max(masked, axis=1)), jnp.float32(-1.0))
    result = lax.map(one_block, (row_groups, order_groups))
    return result.reshape(N)
```

```python
import functools

import jax
import jax.numpy as jnp
from jax import lax
from jax.experimental import pallas as pl
from jax.experimental.pallas import tpu as pltpu
from jax.sharding import PartitionSpec as P

MESH = pl.DeviceIdType.MESH
LANES = 128


def fast_size(rows):
    best = 1
    for size in range(1, rows + 1):
        if rows % size == 0 and size * size <= rows:
            best = size
    return best


class Layout:
    def __init__(self, rows, cols):
        self.fast = fast_size(rows)
        self.slow = rows // self.fast
        self.cores = 2 if cols % 2 == 0 else 1
        self.xs = cols // self.cores
        self.chips = self.fast * self.xs
        self.plane = self.chips * self.cores
        self.top = self.slow - 2 if self.slow > 2 else self.slow - 1
        self.down = self.slow > 2
        chips = [(f, x) for f in range(self.fast) for x in range(self.xs)]
        near = [c for c in chips if (c[0] == 0) != (c[1] == 0)]
        far = [c for c in chips if c[0] != 0 and c[1] != 0]
        self.offsets = near + far
        self.near = list(range(len(near)))
        self.far = list(range(len(near), len(near) + len(far)))
        self.peers = [
            (f, x, c)
            for f in range(self.fast)
            for x in range(self.xs)
            for c in range(self.cores)
            if (f, x, c) != (0, 0, 0)
        ]


def kernel(
    lay, n, chunks,
    emb, order, out,
    units, line, orders, line_orders, col_orders,
    row_best, col_best, plane_res, line_res, plane_in, line_in,
    ps, pr, ss, sr, ls, lr, os_, or_, los, lor, rs, rr, lrs, lrr,
):
    S, F, X, C = lay.slow, lay.fast, lay.xs, lay.cores
    rows_here = n // chunks
    r, c = lax.axis_index("row"), lax.axis_index("col")
    z, f = r // F, lax.rem(r, F)
    x, core = c // C, lax.rem(c, C)
    chip = f * X + x
    slot = chip * C + core

    def plane_id(df, dx, dc):
        return {
            "row": z * F + lax.rem(f + df, F),
            "col": lax.rem(x + dx, X) * C + lax.rem(core + dc, C),
        }

    def line_id(there):
        return {"row": there * F + f, "col": c}

    def source_chip(df, dx):
        return lax.rem(f + F - df, F) * X + lax.rem(x + X - dx, X)

    def span(which, k):
        return pl.ds(pl.multiple_of(which * n + k * rows_here, LANES), rows_here)

    def remote(src, dst, send, recv, where):
        return pltpu.make_async_remote_copy(
            src_ref=src, dst_ref=dst, send_sem=send, recv_sem=recv,
            device_id=where, device_id_type=MESH,
        )

    def plane_copy(i, k):
        part = units.at[span(slot, k)]
        return remote(part, part, ps.at[i, k], pr.at[i, k], plane_id(*lay.offsets[i], 0))

    def sibling_copy(i, k):
        src = chip if i < 0 else source_chip(*lay.offsets[i])
        part = units.at[span(src * C + core, k)]
        return remote(part, part, ss.at[i + 1, k], sr.at[i + 1, k], plane_id(0, 0, 1))

    def plane_wait(i, k):
        src = source_chip(*lay.offsets[i]) * C + core
        part = units.at[span(src, k)]
        remote(part, part, ps.at[i, k], pr.at[i, k], plane_id(*lay.offsets[i], 0)).wait_recv()

    def sibling_wait(i, k):
        src = chip if i < 0 else source_chip(*lay.offsets[i])
        part = units.at[span(src * C + lax.rem(core + 1, C), k)]
        remote(part, part, ss.at[i + 1, k], sr.at[i + 1, k], plane_id(0, 0, 1)).wait_recv()

    def line_copy(src, k, dst_slot, tag, there):
        return remote(
            src, line.at[dst_slot, pl.ds(k * rows_here, rows_here)],
            ls.at[tag, k], lr.at[dst_slot, k], line_id(there),
        )

    def own_part(k):
        return units.at[span(slot, k)]

    base = jnp.minimum(z, lay.top)
    sends_up = z < lay.top
    last = S - 1
    sends_down = (z == last) if lay.down else None
    takes_down = (z == last - 1) if lay.down else None

    def relays(w, k):
        part = line.at[w, pl.ds(k * rows_here, rows_here)]
        found = []
        if w < lay.top:
            found.append(((base >= w) & (z < lay.top), line_copy(part, k, w + 1, w, z + 1)))
        if lay.down:
            found.append(((base >= w) & (z == lay.top), line_copy(part, k, w, w, z + 1)))
        return found

    def order_copy(o):
        return remote(order, orders.at[slot], os_.at[o], or_.at[o], plane_id(*lay.peers[o]))

    def order_wait(o):
        df, dx, dc = lay.peers[o]
        src = source_chip(df, dx) * C + lax.rem(core + C - dc, C)
        remote(order, orders.at[src], os_.at[o], or_.at[o], plane_id(df, dx, dc)).wait_recv()

    def meets(src, dst):
        up = (src < dst) & ((src != lay.top) | (not lay.down))
        if lay.down:
            up = up | ((src == last) & (dst == last - 1))
        return up

    def line_order_copy(dst):
        return remote(order, line_orders.at[z], los.at[dst], lor.at[z], line_id(dst))

    barrier = pltpu.get_barrier_semaphore()
    for peer in lay.peers:
        pl.semaphore_signal(barrier, inc=1, device_id=plane_id(*peer), device_id_type=MESH)
    for dz in range(1, S):
        pl.semaphore_signal(
            barrier, inc=1, device_id=line_id(lax.rem(z + dz, S)), device_id_type=MESH
        )

    for k in range(chunks):
        floats = emb[pl.ds(k * rows_here, rows_here), :].astype(jnp.float32)
        scale = lax.rsqrt(jnp.sum(floats * floats, axis=1, keepdims=True) + 1e-06)
        units[span(slot, k), :] = (floats * scale).astype(jnp.bfloat16)

    row_best[...] = jnp.full(row_best.shape, -1.0, jnp.float32)
    col_best[...] = jnp.full(col_best.shape, -1.0, jnp.float32)
    orders[pl.ds(slot, 1)] = order[...].reshape(1, 1, n)

    def spread(which, row):
        wide = jnp.broadcast_to(row.reshape(1, n), (LANES, n))
        col_orders[which] = wide.T

    spread(lay.top + 1, order[...])
    pl.semaphore_wait(barrier, len(lay.peers) + S - 1)

    for k in range(chunks):
        pl.when(sends_up)(lambda k=k: line_copy(own_part(k), k, 1, lay.top + 1, z + 1).start())
        if lay.down:
            pl.when(sends_down)(lambda k=k: line_copy(own_part(k), k, 0, 0, z - 1).start())
        for i in lay.near:
            plane_copy(i, k).start()
        if C > 1:
            sibling_copy(-1, k).start()
    for o in range(len(lay.peers)):
        order_copy(o).start()
    for dst in range(S):
        pl.when(meets(z, dst))(lambda dst=dst: line_order_copy(dst).start())
    for i in lay.far:
        for k in range(chunks):
            plane_copy(i, k).start()

    width = C * n

    def scores(lhs, which_chip):
        rhs = units[pl.ds(pl.multiple_of(which_chip * width, LANES), width), :]
        return lax.dot_general(
            lhs, rhs, (((1,), (1,)), ((), ())), preferred_element_type=jnp.float32
        )

    def item(lhs, w, which_chip, both, first=0, count=n):
        s = scores(lhs, which_chip)
        mine = col_orders[w, first:first + count, :]
        rows_max = None
        for j in range(width // LANES):
            at = j * LANES
            part = s[:, at:at + LANES]
            core_at, lane_at = at // n, at % n
            theirs = orders[which_chip * C + core_at, :, lane_at:lane_at + LANES]
            earlier = theirs < mine
            if both:
                cand = jnp.where(earlier, part, jnp.float32(-1.0))
                rows_max = cand if rows_max is None else jnp.maximum(rows_max, cand)
                later = jnp.where(earlier, jnp.float32(-1.0), part)
            else:
                later = jnp.where(mine < theirs, part, jnp.float32(-1.0))
            down = jnp.max(later.reshape(count // 8, 8, LANES), axis=0)
            col_best[which_chip, :, at:at + LANES] = jnp.maximum(
                col_best[which_chip, :, at:at + LANES], down
            )
        if both:
            row_best[w, first:first + count, :] = jnp.maximum(
                row_best[w, first:first + count, :], rows_max
            )

    def own_item(which_chip):
        lhs = units[pl.ds(pl.multiple_of(slot * n, LANES), n), :]
        item(lhs, lay.top + 1, which_chip, False)

    def line_item(w, which_chip):
        item(line[w], w, which_chip, True)

    def valid(w):
        return takes_down if w == 0 else base >= w

    early = [w for w in ([0] if lay.down else []) + [1] if w <= lay.top]
    late = list(range(2, lay.top + 1))

    for o in range(len(lay.peers)):
        order_wait(o)
    for w in ([0] if lay.down else []) + list(range(1, lay.top + 1)):
        src = (z + 1) if w == 0 else base - w

        def take(w=w, src=src):
            remote(order, line_orders.at[src], los.at[0], lor.at[src], line_id(z)).wait_recv()
            spread(w, line_orders[src])

        pl.when(valid(w))(take)

    if C > 1:
        for k in range(chunks):
            sibling_wait(-1, k)
    own_item(chip)

    def line_wait(w, k):
        line_copy(line.at[w, pl.ds(k * rows_here, rows_here)], k, w, 0, z).wait_recv()

    def pass_on(w, k):
        pl.when(valid(w))(lambda: line_wait(w, k))
        if w > 0:
            for cond, copy in relays(w, k):
                pl.when(cond)(lambda copy=copy: copy.start())

    for k in range(chunks):
        for w in reversed(early):
            pass_on(w, k)
        for i in lay.near:
            plane_wait(i, k)
            if C > 1:
                sibling_copy(i, k).start()
    if C > 1:
        for i in lay.near:
            for k in range(chunks):
                sibling_wait(i, k)

    near_chips = [source_chip(*lay.offsets[i]) for i in lay.near]
    far_chips = [source_chip(*lay.offsets[i]) for i in lay.far]

    def sweep(ws, chips, own):
        def body(which):
            if own:
                own_item(which)
            for w in ws:
                pl.when(valid(w))(lambda w=w: line_item(w, which))

        for which in chips:
            body(which)

    work = [(early, [chip], False)] + [(early, [one], True) for one in near_chips]
    groups = [work[k::chunks] for k in range(chunks)]
    for k in range(chunks):
        for ws, chips, own in groups[k]:
            sweep(ws, chips, own)
        for w in late:
            pass_on(w, k)
        for i in lay.far:
            plane_wait(i, k)
            if C > 1:
                sibling_copy(i, k).start()
    sweep(late, [chip] + near_chips, False)
    if C > 1:
        for i in lay.far:
            for k in range(chunks):
                sibling_wait(i, k)
    sweep(early + late, far_chips, True)

    for one in range(lay.chips):
        flat = jnp.max(col_best[one], axis=0, keepdims=True)
        for core_at in range(C):
            plane_res[one * C + core_at] = flat[:, core_at * n:(core_at + 1) * n]

    for w in range(lay.top + 1):
        if w == 0 and not lay.down:
            continue

        def fold(w=w):
            line_res[w] = jnp.max(row_best[w].T, axis=0, keepdims=True)

        pl.when(valid(w))(fold)

    def result_copy(o):
        df, dx, dc = lay.peers[o]
        there = (lax.rem(f + df, F) * X + lax.rem(x + dx, X)) * C + lax.rem(core + dc, C)
        return remote(
            plane_res.at[there], plane_in.at[o], rs.at[o], rr.at[o], plane_id(df, dx, dc)
        )

    def line_result(w):
        there = z + 1 if w == 0 else base - w
        return remote(line_res.at[w], line_in.at[z], lrs.at[w], lrr.at[z], line_id(there))

    for w in range(lay.top + 1):
        if w == 0 and not lay.down:
            continue
        pl.when(valid(w))(lambda w=w: line_result(w).start())
    for o in range(len(lay.peers)):
        result_copy(o).start()

    best = jnp.maximum(plane_res[slot], jnp.float32(-1.0))
    for o in range(len(lay.peers)):
        result_copy(o).wait_recv()
        best = jnp.maximum(best, plane_in[o])
    out[...] = best
    for src in range(S):
        def gather(src=src):
            remote(
                line_res.at[0], line_in.at[src], lrs.at[0], lrr.at[src], line_id(z)
            ).wait_recv()
            out[...] = jnp.maximum(out[...], line_in[src])

        pl.when(meets(z, jnp.int32(src)))(gather)

    for k in range(chunks):
        pl.when(sends_up)(lambda k=k: line_copy(own_part(k), k, 1, lay.top + 1, z + 1).wait_send())
        if lay.down:
            pl.when(sends_down)(lambda k=k: line_copy(own_part(k), k, 0, 0, z - 1).wait_send())
        for i in range(len(lay.offsets)):
            plane_copy(i, k).wait_send()
        if C > 1:
            for i in range(-1, len(lay.offsets)):
                sibling_copy(i, k).wait_send()
        for w in range(1, lay.top + 1):
            for cond, copy in relays(w, k):
                pl.when(cond)(lambda copy=copy: copy.wait_send())
    for o in range(len(lay.peers)):
        order_copy(o).wait_send()
        result_copy(o).wait_send()
    for dst in range(S):
        pl.when(meets(z, dst))(lambda dst=dst: line_order_copy(dst).wait_send())
    for w in range(lay.top + 1):
        if w == 0 and not lay.down:
            continue
        pl.when(valid(w))(lambda w=w: line_result(w).wait_send())


def shards(lay, embeddings, doc_order):
    n, depth = embeddings.shape
    chunks = n // LANES if n % LANES == 0 else 1
    dma = pltpu.SemaphoreType.DMA
    near, peers, top, S = len(lay.offsets), len(lay.peers), lay.top, lay.slow
    found = pl.pallas_call(
        functools.partial(kernel, lay, n, chunks),
        out_shape=jax.ShapeDtypeStruct((1, n), jnp.float32),
        in_specs=[pl.BlockSpec(memory_space=pltpu.VMEM)] * 2,
        out_specs=pl.BlockSpec(memory_space=pltpu.VMEM),
        scratch_shapes=[
            pltpu.VMEM((lay.plane * n, depth), jnp.bfloat16),
            pltpu.VMEM((top + 1, n, depth), jnp.bfloat16),
            pltpu.VMEM((lay.plane, 1, n), jnp.int32),
            pltpu.VMEM((S, 1, n), jnp.int32),
            pltpu.VMEM((top + 2, n, LANES), jnp.int32),
            pltpu.VMEM((top + 1, n, LANES), jnp.float32),
            pltpu.VMEM((lay.chips, 8, lay.cores * n), jnp.float32),
            pltpu.VMEM((lay.plane, 1, n), jnp.float32),
            pltpu.VMEM((top + 1, 1, n), jnp.float32),
            pltpu.VMEM((peers, 1, n), jnp.float32),
            pltpu.VMEM((S, 1, n), jnp.float32),
            dma((near, chunks)), dma((near, chunks)),
            dma((near + 1, chunks)), dma((near + 1, chunks)),
            dma((top + 2, chunks)), dma((top + 1, chunks)),
            dma((peers,)), dma((peers,)),
            dma((S,)), dma((S,)),
            dma((peers,)), dma((peers,)),
            dma((top + 1,)), dma((S,)),
        ],
        compiler_params=pltpu.CompilerParams(
            collective_id=0, has_side_effects=True, vmem_limit_bytes=60 * 1024 * 1024
        ),
    )(embeddings, doc_order.reshape(1, n))
    return found.reshape(n)


def solution(mesh):
    lay = Layout(mesh.shape["row"], mesh.shape["col"])
    return jax.shard_map(
        functools.partial(shards, lay),
        mesh=mesh,
        in_specs=(P(("row", "col"), None), P(("row", "col"))),
        out_specs=P(("row", "col")),
        check_vma=False,
    )
```

```python
import functools

import jax
import jax.numpy as jnp
from jax import lax
from jax.experimental import pallas as pl
from jax.experimental.pallas import tpu as pltpu
from jax.sharding import PartitionSpec as P

MESH = pl.DeviceIdType.MESH
LANES = 128
PIECE = 64
GROUP = 128


def fast_size(rows):
    best = 1
    for size in range(1, rows + 1):
        if rows % size == 0 and size * size <= rows:
            best = size
    return best


class Layout:
    def __init__(self, rows, cols):
        self.fast = fast_size(rows)
        self.slow = rows // self.fast
        self.cores = 2 if cols % 2 == 0 else 1
        self.xs = cols // self.cores
        self.chips = self.fast * self.xs
        self.plane = self.chips * self.cores
        self.top = self.slow - 2 if self.slow > 2 else self.slow - 1
        self.down = self.slow > 2
        chips = [(f, x) for f in range(self.fast) for x in range(self.xs)]
        near = [c for c in chips if (c[0] == 0) != (c[1] == 0)]
        far = [c for c in chips if c[0] != 0 and c[1] != 0]
        self.offsets = near + far
        self.near = list(range(len(near)))
        self.far = list(range(len(near), len(near) + len(far)))
        self.peers = [
            (f, x, c)
            for f in range(self.fast)
            for x in range(self.xs)
            for c in range(self.cores)
            if (f, x, c) != (0, 0, 0)
        ]


def kernel(
    lay, n, chunks,
    emb, order, out,
    units, line, orders, line_orders, col_orders,
    row_best, col_best, plane_res, line_res, plane_in, line_in, line_best,
    ps, pr, ss, sr, ls, lr, os_, or_, los, lor, rs, rr, lrs, lrr,
):
    S, F, X, C = lay.slow, lay.fast, lay.xs, lay.cores
    rows_here = n // chunks
    align = PIECE if rows_here % PIECE == 0 else rows_here
    r, c = lax.axis_index("row"), lax.axis_index("col")
    z, f = r // F, lax.rem(r, F)
    x, core = c // C, lax.rem(c, C)
    chip = f * X + x
    slot = chip * C + core

    def plane_id(df, dx, dc):
        return {
            "row": z * F + lax.rem(f + df, F),
            "col": lax.rem(x + dx, X) * C + lax.rem(core + dc, C),
        }

    def line_id(there):
        return {"row": there * F + f, "col": c}

    def source_chip(df, dx):
        return lax.rem(f + F - df, F) * X + lax.rem(x + X - dx, X)

    def span(which, k):
        return pl.ds(pl.multiple_of(which * n + k * rows_here, align), rows_here)

    def remote(src, dst, send, recv, where):
        return pltpu.make_async_remote_copy(
            src_ref=src, dst_ref=dst, send_sem=send, recv_sem=recv,
            device_id=where, device_id_type=MESH,
        )

    def plane_copy(i, k):
        part = units.at[span(slot, k)]
        return remote(part, part, ps.at[i, k], pr.at[i, k], plane_id(*lay.offsets[i], 0))

    def relay_copy(i, k):
        df, dx = lay.offsets[i]
        src, step = ((0, dx), (df, 0)) if k % 2 == 0 else ((df, 0), (0, dx))
        part = units.at[span(source_chip(*src) * C + core, k)]
        return remote(part, part, ps.at[i, k], pr.at[i, k], plane_id(*step, 0))

    def sibling_copy(i, k):
        src = chip if i < 0 else source_chip(*lay.offsets[i])
        part = units.at[span(src * C + core, k)]
        return remote(part, part, ss.at[i + 1, k], sr.at[i + 1, k], plane_id(0, 0, 1))

    def plane_wait(i, k):
        src = source_chip(*lay.offsets[i]) * C + core
        part = units.at[span(src, k)]
        remote(part, part, ps.at[i, k], pr.at[i, k], plane_id(*lay.offsets[i], 0)).wait_recv()

    def sibling_wait(i, k):
        src = chip if i < 0 else source_chip(*lay.offsets[i])
        part = units.at[span(src * C + lax.rem(core + 1, C), k)]
        remote(part, part, ss.at[i + 1, k], sr.at[i + 1, k], plane_id(0, 0, 1)).wait_recv()

    def line_copy(src, k, dst_slot, tag, there):
        return remote(
            src, line.at[dst_slot, pl.ds(k * rows_here, rows_here)],
            ls.at[tag, k], lr.at[dst_slot, k], line_id(there),
        )

    def own_part(k):
        return units.at[span(slot, k)]

    base = jnp.minimum(z, lay.top)
    sends_up = z < lay.top
    last = S - 1
    sends_down = (z == last) if lay.down else None
    takes_down = (z == last - 1) if lay.down else None

    def relays(w, k):
        part = line.at[w, pl.ds(k * rows_here, rows_here)]
        found = []
        if w < lay.top:
            found.append(((base >= w) & (z < lay.top), line_copy(part, k, w + 1, w, z + 1)))
        if lay.down:
            found.append(((base >= w) & (z == lay.top), line_copy(part, k, w, w, z + 1)))
        return found

    def order_copy(o):
        return remote(orders.at[slot], orders.at[slot], os_.at[o], or_.at[o], plane_id(*lay.peers[o]))

    def order_wait(o):
        df, dx, dc = lay.peers[o]
        src = source_chip(df, dx) * C + lax.rem(core + C - dc, C)
        remote(orders.at[slot], orders.at[src], os_.at[o], or_.at[o], plane_id(df, dx, dc)).wait_recv()

    def meets(src, dst):
        up = (src < dst) & ((src != lay.top) | (not lay.down))
        if lay.down:
            up = up | ((src == last) & (dst == last - 1))
        return up

    def line_order_copy(dst):
        return remote(orders.at[slot], line_orders.at[z], los.at[dst], lor.at[z], line_id(dst))

    barrier = pltpu.get_barrier_semaphore()
    for peer in lay.peers:
        pl.semaphore_signal(barrier, inc=1, device_id=plane_id(*peer), device_id_type=MESH)
    for dz in range(1, S):
        pl.semaphore_signal(
            barrier, inc=1, device_id=line_id(lax.rem(z + dz, S)), device_id_type=MESH
        )

    orders[pl.ds(slot, 1)] = order[...].reshape(1, 1, n)

    def spread(which, row):
        wide = jnp.broadcast_to(row.reshape(1, n), (LANES, n))
        col_orders[which] = wide.T

    def normalize(k):
        floats = emb[pl.ds(k * rows_here, rows_here), :].astype(jnp.float32)
        scale = lax.rsqrt(jnp.sum(floats * floats, axis=1, keepdims=True) + 1e-06)
        units[span(slot, k), :] = (floats * scale).astype(jnp.bfloat16)

    def send_own(k):
        pl.when(sends_up)(lambda: line_copy(own_part(k), k, 1, lay.top + 1, z + 1).start())
        if lay.down:
            pl.when(sends_down)(lambda: line_copy(own_part(k), k, 0, 0, z - 1).start())
        for i in lay.near:
            plane_copy(i, k).start()
        if C > 1:
            sibling_copy(-1, k).start()

    for k in range(chunks):
        normalize(k)
    pl.semaphore_wait(barrier, len(lay.peers) + S - 1)
    for dst in range(S):
        pl.when(meets(z, dst))(lambda dst=dst: line_order_copy(dst).start())
    for o in range(len(lay.peers)):
        order_copy(o).start()
    for k in range(chunks):
        send_own(k)

    row_best[...] = jnp.full(row_best.shape, -1.0, jnp.float32)
    col_best[...] = jnp.full(col_best.shape, -1.0, jnp.float32)
    spread(lay.top + 1, order[...].reshape(1, n))

    width = C * n

    def scores(lhs, which_chip):
        rhs = units[pl.ds(pl.multiple_of(which_chip * width, LANES), width), :]
        return lax.dot_general(
            lhs, rhs, (((1,), (1,)), ((), ())), preferred_element_type=jnp.float32
        )

    def item(lhs, w, which_chip, both, first=0, count=n):
        s = scores(lhs, which_chip)
        mine = col_orders[w, first:first + count, :]
        rows_max = None
        for j in range(width // LANES):
            at = j * LANES
            part = s[:, at:at + LANES]
            core_at, lane_at = at // n, at % n
            theirs = orders[which_chip * C + core_at, :, lane_at:lane_at + LANES]
            earlier = theirs < mine
            if both:
                cand = jnp.where(earlier, part, jnp.float32(-1.0))
                rows_max = cand if rows_max is None else jnp.maximum(rows_max, cand)
                later = jnp.where(earlier, jnp.float32(-1.0), part)
            else:
                later = jnp.where(mine < theirs, part, jnp.float32(-1.0))
            down = jnp.max(later.reshape(count // 8, 8, LANES), axis=0)
            col_best[which_chip, :, at:at + LANES] = jnp.maximum(
                col_best[which_chip, :, at:at + LANES], down
            )
        if both:
            row_best[w, first:first + count, :] = jnp.maximum(
                row_best[w, first:first + count, :], rows_max
            )

    def own_item(which_chip):
        lhs = units[pl.ds(pl.multiple_of(slot * n, LANES), n), :]
        item(lhs, lay.top + 1, which_chip, False)

    def line_item(w, which_chip):
        item(line[w], w, which_chip, True)

    def valid(w):
        return takes_down if w == 0 else base >= w

    early = [w for w in ([0] if lay.down else []) + [1] if w <= lay.top]
    late = list(range(2, lay.top + 1))

    for o in range(len(lay.peers)):
        order_wait(o)
    for w in ([0] if lay.down else []) + list(range(1, lay.top + 1)):
        src = (z + 1) if w == 0 else base - w

        def take(w=w, src=src):
            remote(orders.at[slot], line_orders.at[src], los.at[0], lor.at[src], line_id(z)).wait_recv()
            spread(w, line_orders[src])

        pl.when(valid(w))(take)

    if C > 1:
        for k in range(chunks):
            sibling_wait(-1, k)
    own_item(chip)

    def line_wait(w, k):
        line_copy(line.at[w, pl.ds(k * rows_here, rows_here)], k, w, 0, z).wait_recv()

    def pass_on(w, k):
        pl.when(valid(w))(lambda: line_wait(w, k))
        if w > 0:
            for cond, copy in relays(w, k):
                pl.when(cond)(lambda copy=copy: copy.start())

    def chips_of(places):
        def at(j):
            if places == "near":
                by_x = j < X - 1
                df = jnp.where(by_x, 0, j - (X - 2))
                dx = jnp.where(by_x, j + 1, 0)
            elif places == "far":
                df, dx = 1 + j // max(X - 1, 1), 1 + lax.rem(j, max(X - 1, 1))
            elif places == "self":
                df, dx = 0, 0
            else:
                df, dx = j // X, lax.rem(j, X)
            return source_chip(df, dx)

        count = {"near": F + X - 2, "far": (F - 1) * (X - 1), "self": 1, "all": F * X}
        return count[places], at

    def loop(places, body):
        count, at = chips_of(places)

        def step(j, carry):
            body(at(j))
            return carry

        if count:
            lax.fori_loop(0, count, step, 0)

    def own_sweep(places):
        loop(places, own_item)

    def line_sweep(w, places):
        pl.when(valid(w))(lambda: loop(places, lambda one: line_item(w, one)))

    def late_sweep(w, g):
        first = g * group

        def body(one):
            item(line[w, first:first + group, :], w, one, True, first, group)

        pl.when(valid(w))(lambda: loop("all", body))

    group = GROUP if n % GROUP == 0 else n
    groups = n // group
    per = chunks // groups if chunks % groups == 0 else chunks
    if chunks % groups != 0:
        group, groups = n, 1

    for k in range(chunks):
        for w in reversed(early):
            pass_on(w, k)
        for i in lay.near:
            plane_wait(i, k)
        for i in lay.far:
            relay_copy(i, k).start()
        if C > 1:
            for i in lay.near:
                sibling_copy(i, k).start()

    work = [lambda: own_sweep("near")]
    for w in reversed(early):
        work.append(lambda w=w: line_sweep(w, "near"))
        work.append(lambda w=w: line_sweep(w, "self"))
    far_work = [lambda: own_sweep("far")]
    for w in reversed(early):
        far_work.append(lambda w=w: line_sweep(w, "far"))

    half = chunks // 2
    far_pieces = [list(range(2 * k, min(2 * k + 2, chunks))) for k in range(chunks)]
    if half == 0:
        far_pieces = [list(range(chunks))]
    pending = []
    for k in range(chunks):
        for w in late:
            pass_on(w, k)
        for j in far_pieces[k]:
            for i in lay.far:
                plane_wait(i, j)
                if C > 1:
                    sibling_copy(i, j).start()
        if k == 0:
            if C > 1:
                for i in lay.near:
                    for j in range(chunks):
                        sibling_wait(i, j)
            pending += work
        if k == min(half, chunks - 1):
            if C > 1:
                for i in lay.far:
                    for j in range(chunks):
                        sibling_wait(i, j)
            pending += far_work
        if k == min(half, chunks - 1):
            for g in range((k + 1) // per):
                pending += [lambda w=w, g=g: late_sweep(w, g) for w in late]
        elif k > half and (k + 1) % per == 0:
            pending += [lambda w=w, g=(k + 1) // per - 1: late_sweep(w, g) for w in late]
        take = len(pending) if k == chunks - 1 else 2
        for run in pending[:take]:
            run()
        pending = pending[take:]

    for one in range(lay.chips):
        flat = jnp.max(col_best[one], axis=0, keepdims=True)
        for core_at in range(C):
            plane_res[one * C + core_at] = flat[:, core_at * n:(core_at + 1) * n]

    for w in range(lay.top + 1):
        if w == 0 and not lay.down:
            continue

        def fold(w=w):
            line_res[w] = jnp.max(row_best[w].T, axis=0, keepdims=True)

        pl.when(valid(w))(fold)

    def result_copy(o):
        df, dx, dc = lay.peers[o]
        there = (lax.rem(f + df, F) * X + lax.rem(x + dx, X)) * C + lax.rem(core + dc, C)
        return remote(
            plane_res.at[there], plane_in.at[o], rs.at[o], rr.at[o], plane_id(df, dx, dc)
        )

    def line_result(w):
        there = z + 1 if w == 0 else base - w
        return remote(line_res.at[w], line_in.at[z], lrs.at[w], lrr.at[z], line_id(there))

    for w in range(lay.top + 1):
        if w == 0 and not lay.down:
            continue
        pl.when(valid(w))(lambda w=w: line_result(w).start())
    for o in range(len(lay.peers)):
        result_copy(o).start()

    best = jnp.maximum(plane_res[slot], jnp.float32(-1.0))
    for o in range(len(lay.peers)):
        result_copy(o).wait_recv()
        best = jnp.maximum(best, plane_in[o])
    line_best[...] = best.reshape(1, n)
    for src in range(S):
        def gather(src=src):
            remote(
                line_res.at[0], line_in.at[src], lrs.at[0], lrr.at[src], line_id(z)
            ).wait_recv()
            line_best[...] = jnp.maximum(line_best[...], line_in[src])

        pl.when(meets(z, jnp.int32(src)))(gather)

    out[...] = line_best[...].reshape(n)
    for k in range(chunks):
        pl.when(sends_up)(lambda k=k: line_copy(own_part(k), k, 1, lay.top + 1, z + 1).wait_send())
        if lay.down:
            pl.when(sends_down)(lambda k=k: line_copy(own_part(k), k, 0, 0, z - 1).wait_send())
        for i in lay.near:
            plane_copy(i, k).wait_send()
        for i in lay.far:
            relay_copy(i, k).wait_send()
        if C > 1:
            for i in range(-1, len(lay.offsets)):
                sibling_copy(i, k).wait_send()
        for w in range(1, lay.top + 1):
            for cond, copy in relays(w, k):
                pl.when(cond)(lambda copy=copy: copy.wait_send())
    for o in range(len(lay.peers)):
        order_copy(o).wait_send()
        result_copy(o).wait_send()
    for dst in range(S):
        pl.when(meets(z, dst))(lambda dst=dst: line_order_copy(dst).wait_send())
    for w in range(lay.top + 1):
        if w == 0 and not lay.down:
            continue
        pl.when(valid(w))(lambda w=w: line_result(w).wait_send())


def shards(lay, embeddings, doc_order):
    n, depth = embeddings.shape
    chunks = n // PIECE if n % PIECE == 0 else 1
    dma = pltpu.SemaphoreType.DMA
    near, peers, top, S = len(lay.offsets), len(lay.peers), lay.top, lay.slow
    found = pl.pallas_call(
        functools.partial(kernel, lay, n, chunks),
        out_shape=jax.ShapeDtypeStruct((n,), jnp.float32),
        in_specs=[pl.BlockSpec(memory_space=pltpu.VMEM)] * 2,
        out_specs=pl.BlockSpec(memory_space=pltpu.VMEM),
        scratch_shapes=[
            pltpu.VMEM((lay.plane * n, depth), jnp.bfloat16),
            pltpu.VMEM((top + 1, n, depth), jnp.bfloat16),
            pltpu.VMEM((lay.plane, 1, n), jnp.int32),
            pltpu.VMEM((S, 1, n), jnp.int32),
            pltpu.VMEM((top + 2, n, LANES), jnp.int32),
            pltpu.VMEM((top + 1, n, LANES), jnp.float32),
            pltpu.VMEM((lay.chips, 8, lay.cores * n), jnp.float32),
            pltpu.VMEM((lay.plane, 1, n), jnp.float32),
            pltpu.VMEM((top + 1, 1, n), jnp.float32),
            pltpu.VMEM((peers, 1, n), jnp.float32),
            pltpu.VMEM((S, 1, n), jnp.float32),
            pltpu.VMEM((1, n), jnp.float32),
            dma((near, chunks)), dma((near, chunks)),
            dma((near + 1, chunks)), dma((near + 1, chunks)),
            dma((top + 2, chunks)), dma((top + 1, chunks)),
            dma((peers,)), dma((peers,)),
            dma((S,)), dma((S,)),
            dma((peers,)), dma((peers,)),
            dma((top + 1,)), dma((S,)),
        ],
        compiler_params=pltpu.CompilerParams(
            collective_id=0, has_side_effects=True, vmem_limit_bytes=60 * 1024 * 1024
        ),
    )(embeddings, doc_order)
    return found


def solution(mesh):
    lay = Layout(mesh.shape["row"], mesh.shape["col"])
    return jax.shard_map(
        functools.partial(shards, lay),
        mesh=mesh,
        in_specs=(P(("row", "col"), None), P(("row", "col"))),
        out_specs=P(("row", "col")),
        check_vma=False,
    )
```

```python
import functools

import jax
import jax.numpy as jnp
from jax import lax
from jax.experimental import pallas as pl
from jax.experimental.pallas import tpu as pltpu
from jax.sharding import PartitionSpec as P

MESH = pl.DeviceIdType.MESH
LANES = 128
PIECE = 64
GROUP = 128


def fast_size(rows):
    best = 1
    for size in range(1, rows + 1):
        if rows % size == 0 and size * size <= rows:
            best = size
    return best


class Layout:
    def __init__(self, rows, cols):
        self.fast = fast_size(rows)
        self.slow = rows // self.fast
        self.cores = 2 if cols % 2 == 0 else 1
        self.xs = cols // self.cores
        self.chips = self.fast * self.xs
        self.plane = self.chips * self.cores
        self.top = self.slow - 2 if self.slow > 2 else self.slow - 1
        self.down = self.slow > 2
        chips = [(f, x) for f in range(self.fast) for x in range(self.xs)]
        near = [c for c in chips if (c[0] == 0) != (c[1] == 0)]
        far = [c for c in chips if c[0] != 0 and c[1] != 0]
        self.offsets = near + far
        self.near = list(range(len(near)))
        self.far = list(range(len(near), len(near) + len(far)))
        self.peers = [
            (f, x, c)
            for f in range(self.fast)
            for x in range(self.xs)
            for c in range(self.cores)
            if (f, x, c) != (0, 0, 0)
        ]


def kernel(
    lay, n, chunks,
    emb, order, out,
    units, line, orders, line_orders, col_orders,
    row_best, col_best, plane_res, line_res, plane_in, line_in, line_best,
    ps, pr, ss, sr, ls, lr, os_, or_, los, lor, rs, rr, lrs, lrr,
):
    S, F, X, C = lay.slow, lay.fast, lay.xs, lay.cores
    rows_here = n // chunks
    align = PIECE if rows_here % PIECE == 0 else rows_here
    r, c = lax.axis_index("row"), lax.axis_index("col")
    z, f = r // F, lax.rem(r, F)
    x, core = c // C, lax.rem(c, C)
    chip = f * X + x
    slot = chip * C + core

    def plane_id(df, dx, dc):
        return {
            "row": z * F + lax.rem(f + df, F),
            "col": lax.rem(x + dx, X) * C + lax.rem(core + dc, C),
        }

    def line_id(there):
        return {"row": there * F + f, "col": c}

    def source_chip(df, dx):
        return lax.rem(f + F - df, F) * X + lax.rem(x + X - dx, X)

    def span(which, k):
        return pl.ds(pl.multiple_of(which * n + k * rows_here, align), rows_here)

    def remote(src, dst, send, recv, where):
        return pltpu.make_async_remote_copy(
            src_ref=src, dst_ref=dst, send_sem=send, recv_sem=recv,
            device_id=where, device_id_type=MESH,
        )

    def plane_copy(i, k):
        part = units.at[span(slot, k)]
        return remote(part, part, ps.at[i, k], pr.at[i, k], plane_id(*lay.offsets[i], 0))

    def relay_copy(i, k):
        df, dx = lay.offsets[i]
        src, step = ((0, dx), (df, 0)) if k % 2 == 0 else ((df, 0), (0, dx))
        part = units.at[span(source_chip(*src) * C + core, k)]
        return remote(part, part, ps.at[i, k], pr.at[i, k], plane_id(*step, 0))

    def sibling_copy(i, k):
        src = chip if i < 0 else source_chip(*lay.offsets[i])
        part = units.at[span(src * C + core, k)]
        return remote(part, part, ss.at[i + 1, k], sr.at[i + 1, k], plane_id(0, 0, 1))

    def plane_wait(i, k):
        src = source_chip(*lay.offsets[i]) * C + core
        part = units.at[span(src, k)]
        remote(part, part, ps.at[i, k], pr.at[i, k], plane_id(*lay.offsets[i], 0)).wait_recv()

    def sibling_wait(i, k):
        src = chip if i < 0 else source_chip(*lay.offsets[i])
        part = units.at[span(src * C + lax.rem(core + 1, C), k)]
        remote(part, part, ss.at[i + 1, k], sr.at[i + 1, k], plane_id(0, 0, 1)).wait_recv()

    def line_copy(src, k, dst_slot, tag, there):
        return remote(
            src, line.at[dst_slot, pl.ds(k * rows_here, rows_here)],
            ls.at[tag, k], lr.at[dst_slot, k], line_id(there),
        )

    def own_part(k):
        return units.at[span(slot, k)]

    base = jnp.minimum(z, lay.top)
    sends_up = z < lay.top
    last = S - 1
    sends_down = (z == last) if lay.down else None
    takes_down = (z == last - 1) if lay.down else None

    def relays(w, k):
        part = line.at[w, pl.ds(k * rows_here, rows_here)]
        found = []
        if w < lay.top:
            found.append(((base >= w) & (z < lay.top), line_copy(part, k, w + 1, w, z + 1)))
        if lay.down:
            found.append(((base >= w) & (z == lay.top), line_copy(part, k, w, w, z + 1)))
        return found

    def order_copy(o):
        return remote(orders.at[slot], orders.at[slot], os_.at[o], or_.at[o], plane_id(*lay.peers[o]))

    def order_wait(o):
        df, dx, dc = lay.peers[o]
        src = source_chip(df, dx) * C + lax.rem(core + C - dc, C)
        remote(orders.at[slot], orders.at[src], os_.at[o], or_.at[o], plane_id(df, dx, dc)).wait_recv()

    def meets(src, dst):
        up = (src < dst) & ((src != lay.top) | (not lay.down))
        if lay.down:
            up = up | ((src == last) & (dst == last - 1))
        return up

    def line_order_copy(dst):
        return remote(orders.at[slot], line_orders.at[z], los.at[dst], lor.at[z], line_id(dst))

    barrier = pltpu.get_barrier_semaphore()
    for peer in lay.peers:
        pl.semaphore_signal(barrier, inc=1, device_id=plane_id(*peer), device_id_type=MESH)
    for dz in range(1, S):
        pl.semaphore_signal(
            barrier, inc=1, device_id=line_id(lax.rem(z + dz, S)), device_id_type=MESH
        )

    orders[pl.ds(slot, 1)] = order[...].reshape(1, 1, n)

    def spread(which, row):
        wide = jnp.broadcast_to(row.reshape(1, n), (LANES, n))
        col_orders[which] = wide.T

    def normalize(k):
        floats = emb[pl.ds(k * rows_here, rows_here), :].astype(jnp.float32)
        scale = lax.rsqrt(jnp.sum(floats * floats, axis=1, keepdims=True) + 1e-06)
        units[span(slot, k), :] = (floats * scale).astype(jnp.bfloat16)

    def send_own(k):
        pl.when(sends_up)(lambda: line_copy(own_part(k), k, 1, lay.top + 1, z + 1).start())
        if lay.down:
            pl.when(sends_down)(lambda: line_copy(own_part(k), k, 0, 0, z - 1).start())
        for i in lay.near:
            plane_copy(i, k).start()
        if C > 1:
            sibling_copy(-1, k).start()

    for k in range(chunks):
        normalize(k)
    pl.semaphore_wait(barrier, len(lay.peers) + S - 1)
    for dst in range(S):
        pl.when(meets(z, dst))(lambda dst=dst: line_order_copy(dst).start())
    for o in range(len(lay.peers)):
        order_copy(o).start()
    for k in range(chunks):
        send_own(k)

    row_best[...] = jnp.full(row_best.shape, -1.0, jnp.float32)
    col_best[...] = jnp.full(col_best.shape, -1.0, jnp.float32)
    spread(lay.top + 1, order[...].reshape(1, n))

    width = C * n

    def item(lhs, w, first_chip, both, first=0, count=n, wide=1):
        rhs = units[pl.ds(pl.multiple_of(first_chip * width, LANES), wide * width), :]
        s = lax.dot_general(
            lhs, rhs, (((1,), (1,)), ((), ())), preferred_element_type=jnp.float32
        )
        mine = col_orders[w, first:first + count, :]
        rows_max = None
        for j in range(wide * width // LANES):
            part = s[:, j * LANES:(j + 1) * LANES]
            which_chip, at = first_chip + j * LANES // width, j * LANES % width
            core_at, lane_at = at // n, at % n
            theirs = orders[which_chip * C + core_at, :, lane_at:lane_at + LANES]
            earlier = theirs < mine
            if both:
                cand = jnp.where(earlier, part, jnp.float32(-1.0))
                rows_max = cand if rows_max is None else jnp.maximum(rows_max, cand)
                later = jnp.where(earlier, jnp.float32(-1.0), part)
            else:
                later = jnp.where(mine < theirs, part, jnp.float32(-1.0))
            down = jnp.max(later.reshape(count // 8, 8, LANES), axis=0)
            col_best[which_chip, :, at:at + LANES] = jnp.maximum(
                col_best[which_chip, :, at:at + LANES], down
            )
        if both:
            row_best[w, first:first + count, :] = jnp.maximum(
                row_best[w, first:first + count, :], rows_max
            )

    def own_item(which_chip):
        lhs = units[pl.ds(pl.multiple_of(slot * n, LANES), n), :]
        item(lhs, lay.top + 1, which_chip, False)

    def line_item(w, which_chip):
        item(line[w], w, which_chip, True)

    def valid(w):
        return takes_down if w == 0 else base >= w

    early = [w for w in ([0] if lay.down else []) + [1] if w <= lay.top]
    late = list(range(2, lay.top + 1))

    for o in range(len(lay.peers)):
        order_wait(o)
    for w in ([0] if lay.down else []) + list(range(1, lay.top + 1)):
        src = (z + 1) if w == 0 else base - w

        def take(w=w, src=src):
            remote(orders.at[slot], line_orders.at[src], los.at[0], lor.at[src], line_id(z)).wait_recv()
            spread(w, line_orders[src])

        pl.when(valid(w))(take)

    if C > 1:
        for k in range(chunks):
            sibling_wait(-1, k)
    own_item(chip)

    def line_wait(w, k):
        line_copy(line.at[w, pl.ds(k * rows_here, rows_here)], k, w, 0, z).wait_recv()

    def pass_on(w, k):
        pl.when(valid(w))(lambda: line_wait(w, k))
        if w > 0:
            for cond, copy in relays(w, k):
                pl.when(cond)(lambda copy=copy: copy.start())

    def chips_of(places):
        def at(j):
            if places == "near":
                by_x = j < X - 1
                df = jnp.where(by_x, 0, j - (X - 2))
                dx = jnp.where(by_x, j + 1, 0)
            elif places == "far":
                df, dx = 1 + j // max(X - 1, 1), 1 + lax.rem(j, max(X - 1, 1))
            elif places == "home":
                df, dx = jnp.where(j < X, 0, j - (X - 1)), jnp.where(j < X, j, 0)
            else:
                df, dx = j // X, lax.rem(j, X)
            return source_chip(df, dx)

        count = {"near": F + X - 2, "far": (F - 1) * (X - 1), "home": F + X - 1, "all": F * X}
        return count[places], at

    def loop(places, body):
        count, at = chips_of(places)

        def step(j, carry):
            body(at(j))
            return carry

        if count:
            lax.fori_loop(0, count, step, 0)

    def own_sweep(places):
        loop(places, own_item)

    def line_sweep(w, places):
        pl.when(valid(w))(lambda: loop(places, lambda one: line_item(w, one)))

    wide = next(m for m in (4, 3, 2, 1) if lay.chips % m == 0)

    def late_sweep(w, first, count):
        def body(j, carry):
            item(line[w, first:first + count, :], w, j * wide, True, first, count, wide)
            return carry

        @pl.when(valid(w))
        def run():
            lax.fori_loop(0, lay.chips // wide, body, 0)

    for k in range(chunks):
        for w in reversed(early):
            pass_on(w, k)
        for i in lay.near:
            plane_wait(i, k)
        for i in lay.far:
            relay_copy(i, k).start()
        if C > 1:
            for i in lay.near:
                sibling_copy(i, k).start()

    def when_at(sixths):
        return min(chunks * sixths // 6, chunks - 1)

    plan = [[] for _ in range(chunks)]
    plan[when_at(0)].append(lambda: own_sweep("near"))
    for place, sixths in (("home", 1), ("far", 3)):
        for j, w in enumerate(reversed(early)):
            plan[when_at(sixths + j)].append(lambda w=w, place=place: line_sweep(w, place))
    plan[when_at(3)].append(lambda: own_sweep("far"))
    split = n * 2 // 3 if chunks % 6 == 0 and n * 2 // 3 % GROUP == 0 else 0
    for w in late:
        if split:
            plan[when_at(4)].append(lambda w=w: late_sweep(w, 0, split))
        plan[chunks - 1].append(lambda w=w: late_sweep(w, split, n - split))
    far_pieces = [list(range(2 * k, min(2 * k + 2, chunks))) for k in range(chunks)]
    if chunks == 1:
        far_pieces = [[0]]
    for k in range(chunks):
        for w in late:
            pass_on(w, k)
        for j in far_pieces[k]:
            for i in lay.far:
                plane_wait(i, j)
                if C > 1:
                    sibling_copy(i, j).start()
        if C > 1 and k == 0:
            for i in lay.near:
                for j in range(chunks):
                    sibling_wait(i, j)
        if C > 1 and k == when_at(3):
            for i in lay.far:
                for j in range(chunks):
                    sibling_wait(i, j)
        for run in plan[k]:
            run()

    for one in range(lay.chips):
        flat = jnp.max(col_best[one], axis=0, keepdims=True)
        for core_at in range(C):
            plane_res[one * C + core_at] = flat[:, core_at * n:(core_at + 1) * n]

    for w in range(lay.top + 1):
        if w == 0 and not lay.down:
            continue

        def fold(w=w):
            line_res[w] = jnp.max(row_best[w].T, axis=0, keepdims=True)

        pl.when(valid(w))(fold)

    def result_copy(o):
        df, dx, dc = lay.peers[o]
        there = (lax.rem(f + df, F) * X + lax.rem(x + dx, X)) * C + lax.rem(core + dc, C)
        return remote(
            plane_res.at[there], plane_in.at[o], rs.at[o], rr.at[o], plane_id(df, dx, dc)
        )

    def line_result(w):
        there = z + 1 if w == 0 else base - w
        return remote(line_res.at[w], line_in.at[z], lrs.at[w], lrr.at[z], line_id(there))

    for w in range(lay.top + 1):
        if w == 0 and not lay.down:
            continue
        pl.when(valid(w))(lambda w=w: line_result(w).start())
    for o in range(len(lay.peers)):
        result_copy(o).start()

    best = jnp.maximum(plane_res[slot], jnp.float32(-1.0))
    for o in range(len(lay.peers)):
        result_copy(o).wait_recv()
        best = jnp.maximum(best, plane_in[o])
    line_best[...] = best.reshape(1, n)
    for src in range(S):
        def gather(src=src):
            remote(
                line_res.at[0], line_in.at[src], lrs.at[0], lrr.at[src], line_id(z)
            ).wait_recv()
            line_best[...] = jnp.maximum(line_best[...], line_in[src])

        pl.when(meets(z, jnp.int32(src)))(gather)

    out[...] = line_best[...].reshape(n)
    for k in range(chunks):
        pl.when(sends_up)(lambda k=k: line_copy(own_part(k), k, 1, lay.top + 1, z + 1).wait_send())
        if lay.down:
            pl.when(sends_down)(lambda k=k: line_copy(own_part(k), k, 0, 0, z - 1).wait_send())
        for i in lay.near:
            plane_copy(i, k).wait_send()
        for i in lay.far:
            relay_copy(i, k).wait_send()
        if C > 1:
            for i in range(-1, len(lay.offsets)):
                sibling_copy(i, k).wait_send()
        for w in range(1, lay.top + 1):
            for cond, copy in relays(w, k):
                pl.when(cond)(lambda copy=copy: copy.wait_send())
    for o in range(len(lay.peers)):
        order_copy(o).wait_send()
        result_copy(o).wait_send()
    for dst in range(S):
        pl.when(meets(z, dst))(lambda dst=dst: line_order_copy(dst).wait_send())
    for w in range(lay.top + 1):
        if w == 0 and not lay.down:
            continue
        pl.when(valid(w))(lambda w=w: line_result(w).wait_send())


def shards(lay, embeddings, doc_order):
    n, depth = embeddings.shape
    chunks = n // PIECE if n % PIECE == 0 else 1
    dma = pltpu.SemaphoreType.DMA
    near, peers, top, S = len(lay.offsets), len(lay.peers), lay.top, lay.slow
    found = pl.pallas_call(
        functools.partial(kernel, lay, n, chunks),
        out_shape=jax.ShapeDtypeStruct((n,), jnp.float32),
        in_specs=[pl.BlockSpec(memory_space=pltpu.VMEM)] * 2,
        out_specs=pl.BlockSpec(memory_space=pltpu.VMEM),
        scratch_shapes=[
            pltpu.VMEM((lay.plane * n, depth), jnp.bfloat16),
            pltpu.VMEM((top + 1, n, depth), jnp.bfloat16),
            pltpu.VMEM((lay.plane, 1, n), jnp.int32),
            pltpu.VMEM((S, 1, n), jnp.int32),
            pltpu.VMEM((top + 2, n, LANES), jnp.int32),
            pltpu.VMEM((top + 1, n, LANES), jnp.float32),
            pltpu.VMEM((lay.chips, 8, lay.cores * n), jnp.float32),
            pltpu.VMEM((lay.plane, 1, n), jnp.float32),
            pltpu.VMEM((top + 1, 1, n), jnp.float32),
            pltpu.VMEM((peers, 1, n), jnp.float32),
            pltpu.VMEM((S, 1, n), jnp.float32),
            pltpu.VMEM((1, n), jnp.float32),
            dma((near, chunks)), dma((near, chunks)),
            dma((near + 1, chunks)), dma((near + 1, chunks)),
            dma((top + 2, chunks)), dma((top + 1, chunks)),
            dma((peers,)), dma((peers,)),
            dma((S,)), dma((S,)),
            dma((peers,)), dma((peers,)),
            dma((top + 1,)), dma((S,)),
        ],
        compiler_params=pltpu.CompilerParams(
            collective_id=0, has_side_effects=True, vmem_limit_bytes=60 * 1024 * 1024
        ),
    )(embeddings, doc_order)
    return found


def solution(mesh):
    lay = Layout(mesh.shape["row"], mesh.shape["col"])
    return jax.shard_map(
        functools.partial(shards, lay),
        mesh=mesh,
        in_specs=(P(("row", "col"), None), P(("row", "col"))),
        out_specs=P(("row", "col")),
        check_vma=False,
    )
```

```python
import functools

import jax
import jax.numpy as jnp
from jax import lax
from jax.experimental import pallas as pl
from jax.experimental.pallas import tpu as pltpu
from jax.sharding import PartitionSpec as P

MESH = pl.DeviceIdType.MESH
LANES = 128
PIECE = 64
GROUP = 128


def fast_size(rows):
    best = 1
    for size in range(1, rows + 1):
        if rows % size == 0 and size * size <= rows:
            best = size
    return best


class Layout:
    def __init__(self, rows, cols):
        self.fast = fast_size(rows)
        self.slow = rows // self.fast
        self.cores = 2 if cols % 2 == 0 else 1
        self.xs = cols // self.cores
        self.chips = self.fast * self.xs
        self.plane = self.chips * self.cores
        self.top = self.slow - 2 if self.slow > 2 else self.slow - 1
        self.down = self.slow > 2
        chips = [(f, x) for f in range(self.fast) for x in range(self.xs)]
        near = [c for c in chips if (c[0] == 0) != (c[1] == 0)]
        far = [c for c in chips if c[0] != 0 and c[1] != 0]
        self.offsets = near + far
        self.near = list(range(len(near)))
        self.far = list(range(len(near), len(near) + len(far)))
        self.peers = [
            (f, x, c)
            for f in range(self.fast)
            for x in range(self.xs)
            for c in range(self.cores)
            if (f, x, c) != (0, 0, 0)
        ]


def kernel(
    lay, n, chunks,
    emb, order, out,
    units, line, orders, line_orders, col_orders,
    row_best, col_best, plane_res, line_res, plane_in, line_in, line_best,
    ps, pr, ss, sr, ls, lr, os_, or_, los, lor, oss, osr, rs, rr, lrs, lrr,
):
    S, F, X, C = lay.slow, lay.fast, lay.xs, lay.cores
    rows_here = n // chunks
    align = PIECE if rows_here % PIECE == 0 else rows_here
    r, c = lax.axis_index("row"), lax.axis_index("col")
    z, f = r // F, lax.rem(r, F)
    x, core = c // C, lax.rem(c, C)
    chip = f * X + x
    slot = chip * C + core

    def plane_id(df, dx, dc):
        return {
            "row": z * F + lax.rem(f + df, F),
            "col": lax.rem(x + dx, X) * C + lax.rem(core + dc, C),
        }

    def line_id(there):
        return {"row": there * F + f, "col": c}

    def source_chip(df, dx):
        return lax.rem(f + F - df, F) * X + lax.rem(x + X - dx, X)

    def span(which, k):
        return pl.ds(pl.multiple_of(which * n + k * rows_here, align), rows_here)

    def remote(src, dst, send, recv, where):
        return pltpu.make_async_remote_copy(
            src_ref=src, dst_ref=dst, send_sem=send, recv_sem=recv,
            device_id=where, device_id_type=MESH,
        )

    def plane_copy(i, k):
        part = units.at[span(slot, k)]
        return remote(part, part, ps.at[i, k], pr.at[i, k], plane_id(*lay.offsets[i], 0))

    def relay_copy(i, k):
        df, dx = lay.offsets[i]
        src, step = ((0, dx), (df, 0)) if k % 2 == 0 else ((df, 0), (0, dx))
        part = units.at[span(source_chip(*src) * C + core, k)]
        return remote(part, part, ps.at[i, k], pr.at[i, k], plane_id(*step, 0))

    def sibling_copy(i, k):
        src = chip if i < 0 else source_chip(*lay.offsets[i])
        part = units.at[span(src * C + core, k)]
        return remote(part, part, ss.at[i + 1, k], sr.at[i + 1, k], plane_id(0, 0, 1))

    def plane_wait(i, k):
        src = source_chip(*lay.offsets[i]) * C + core
        part = units.at[span(src, k)]
        remote(part, part, ps.at[i, k], pr.at[i, k], plane_id(*lay.offsets[i], 0)).wait_recv()

    def sibling_wait(i, k):
        src = chip if i < 0 else source_chip(*lay.offsets[i])
        part = units.at[span(src * C + lax.rem(core + 1, C), k)]
        remote(part, part, ss.at[i + 1, k], sr.at[i + 1, k], plane_id(0, 0, 1)).wait_recv()

    def line_copy(src, k, dst_slot, tag, there):
        return remote(
            src, line.at[dst_slot, pl.ds(k * rows_here, rows_here)],
            ls.at[tag, k], lr.at[dst_slot, k], line_id(there),
        )

    def own_part(k):
        return units.at[span(slot, k)]

    base = jnp.minimum(z, lay.top)
    sends_up = z < lay.top
    last = S - 1
    sends_down = (z == last) if lay.down else None
    takes_down = (z == last - 1) if lay.down else None

    def relays(w, k):
        part = line.at[w, pl.ds(k * rows_here, rows_here)]
        found = []
        if w < lay.top:
            found.append(((base >= w) & (z < lay.top), line_copy(part, k, w + 1, w, z + 1)))
        if lay.down:
            found.append(((base >= w) & (z == lay.top), line_copy(part, k, w, w, z + 1)))
        return found

    def order_send(src, i, where):
        return remote(orders.at[src], orders.at[src], os_.at[i], or_.at[i], where)

    def order_copy(i):
        return order_send(slot, i, plane_id(*lay.offsets[i], 0))

    def order_relay(i):
        df, dx = lay.offsets[i]
        return order_send(source_chip(0, dx) * C + core, i, plane_id(df, 0, 0))

    def order_wait(i):
        order_send(source_chip(*lay.offsets[i]) * C + core, i, plane_id(0, 0, 1)).wait_recv()

    def order_across(i, side):
        src = chip if i < 0 else source_chip(*lay.offsets[i])
        part = orders.at[src * C + lax.rem(core + side, C)]
        return remote(part, part, oss.at[i + 1], osr.at[i + 1], plane_id(0, 0, 1))

    def meets(src, dst):
        up = (src < dst) & ((src != lay.top) | (not lay.down))
        if lay.down:
            up = up | ((src == last) & (dst == last - 1))
        return up

    def line_order_copy(part, src, tag, there):
        return remote(part, line_orders.at[src], los.at[tag], lor.at[src], line_id(there))

    def own_order(there):
        return line_order_copy(orders.at[slot], z, 0, there)

    def order_up(w):
        return line_order_copy(line_orders.at[base - w], base - w, w, z + 1)

    def goes_on(w):
        return (base >= w) & (z < last) & (lay.down | (z < lay.top))

    barrier = pltpu.get_barrier_semaphore()
    steps = [(*lay.offsets[i], 0) for i in lay.near] + ([(0, 0, 1)] if C > 1 else [])
    sides = ((z > 0, z - 1), (z < last, z + 1))
    for step in steps:
        pl.semaphore_signal(barrier, inc=1, device_id=plane_id(*step), device_id_type=MESH)
    for there, which in sides:
        pl.when(there)(
            lambda which=which: pl.semaphore_signal(
                barrier, inc=1, device_id=line_id(which), device_id_type=MESH
            )
        )

    orders[pl.ds(slot, 1)] = order[...].reshape(1, 1, n)

    def spread(which, row):
        wide = jnp.broadcast_to(row.reshape(1, n), (LANES, n))
        col_orders[which] = wide.T

    def normalize(k):
        floats = emb[pl.ds(k * rows_here, rows_here), :].astype(jnp.float32)
        scale = lax.rsqrt(jnp.sum(floats * floats, axis=1, keepdims=True) + 1e-06)
        units[span(slot, k), :] = (floats * scale).astype(jnp.bfloat16)

    def send_own(k):
        pl.when(sends_up)(lambda: line_copy(own_part(k), k, 1, lay.top + 1, z + 1).start())
        if lay.down:
            pl.when(sends_down)(lambda: line_copy(own_part(k), k, 0, 0, z - 1).start())
        for i in lay.near:
            plane_copy(i, k).start()
        if C > 1:
            sibling_copy(-1, k).start()

    for k in range(chunks):
        normalize(k)
    lines = jnp.minimum(z, 1) + jnp.minimum(last - z, 1)
    pl.semaphore_wait(barrier, len(steps) + lines)
    pl.when(sends_up)(lambda: own_order(z + 1).start())
    if lay.down:
        pl.when(sends_down)(lambda: own_order(z - 1).start())
    for i in lay.near:
        order_copy(i).start()
    if C > 1:
        order_across(-1, 0).start()
    for k in range(chunks):
        send_own(k)

    row_best[...] = jnp.full(row_best.shape, -1.0, jnp.float32)
    col_best[...] = jnp.full(col_best.shape, -1.0, jnp.float32)
    spread(lay.top + 1, order[...].reshape(1, n))

    width = C * n

    def item(lhs, w, first_chip, both, first=0, count=n, wide=1):
        rhs = units[pl.ds(pl.multiple_of(first_chip * width, LANES), wide * width), :]
        s = lax.dot_general(
            lhs, rhs, (((1,), (1,)), ((), ())), preferred_element_type=jnp.float32
        )
        mine = col_orders[w, first:first + count, :]
        rows_max = None
        for j in range(wide * width // LANES):
            part = s[:, j * LANES:(j + 1) * LANES]
            which_chip, at = first_chip + j * LANES // width, j * LANES % width
            core_at, lane_at = at // n, at % n
            theirs = orders[which_chip * C + core_at, :, lane_at:lane_at + LANES]
            earlier = theirs < mine
            if both:
                cand = jnp.where(earlier, part, jnp.float32(-1.0))
                rows_max = cand if rows_max is None else jnp.maximum(rows_max, cand)
                later = jnp.where(earlier, jnp.float32(-1.0), part)
            else:
                later = jnp.where(mine < theirs, part, jnp.float32(-1.0))
            down = jnp.max(later.reshape(count // 8, 8, LANES), axis=0)
            col_best[which_chip, :, at:at + LANES] = jnp.maximum(
                col_best[which_chip, :, at:at + LANES], down
            )
        if both:
            row_best[w, first:first + count, :] = jnp.maximum(
                row_best[w, first:first + count, :], rows_max
            )

    def own_item(which_chip):
        lhs = units[pl.ds(pl.multiple_of(slot * n, LANES), n), :]
        item(lhs, lay.top + 1, which_chip, False)

    def line_item(w, which_chip):
        item(line[w], w, which_chip, True)

    def valid(w):
        return takes_down if w == 0 else base >= w

    early = [w for w in ([0] if lay.down else []) + [1] if w <= lay.top]
    late = list(range(2, lay.top + 1))

    def take_order(w):
        src = (z + 1) if w == 0 else base - w
        line_order_copy(line_orders.at[src], src, 0, z).wait_recv()
        if w > 0:
            pl.when(goes_on(w))(lambda: order_up(w).start())
        spread(w, line_orders[src])

    for i in lay.near:
        order_wait(i)
        if C > 1:
            order_across(i, 0).start()
    for i in lay.far:
        order_relay(i).start()
    if C > 1:
        order_across(-1, 1).wait_recv()
        for k in range(chunks):
            sibling_wait(-1, k)
    own_item(chip)
    if C > 1:
        for i in lay.near:
            order_across(i, 1).wait_recv()

    def line_wait(w, k):
        line_copy(line.at[w, pl.ds(k * rows_here, rows_here)], k, w, 0, z).wait_recv()

    def pass_on(w, k):
        if k == 0:
            pl.when(valid(w))(lambda: take_order(w))
        pl.when(valid(w))(lambda: line_wait(w, k))
        if w > 0:
            for cond, copy in relays(w, k):
                pl.when(cond)(lambda copy=copy: copy.start())

    def chips_of(places):
        def at(j):
            if places == "near":
                by_x = j < X - 1
                df = jnp.where(by_x, 0, j - (X - 2))
                dx = jnp.where(by_x, j + 1, 0)
            elif places == "far":
                df, dx = 1 + j // max(X - 1, 1), 1 + lax.rem(j, max(X - 1, 1))
            elif places == "self":
                df, dx = 0, 0
            else:
                df, dx = j // X, lax.rem(j, X)
            return source_chip(df, dx)

        count = {"near": F + X - 2, "far": (F - 1) * (X - 1), "self": 1, "all": F * X}
        return count[places], at

    def loop(places, body):
        count, at = chips_of(places)

        def step(j, carry):
            body(at(j))
            return carry

        if count:
            lax.fori_loop(0, count, step, 0)

    def own_sweep(places):
        loop(places, own_item)

    def line_sweep(w, places):
        pl.when(valid(w))(lambda: loop(places, lambda one: line_item(w, one)))

    wide = next(m for m in (4, 3, 2, 1) if lay.chips % m == 0)

    def late_sweep(w, first, count, here):
        def body(j, carry):
            item(line[w, first:first + count, :], w, j * wide, True, first, count, wide)
            return carry

        @pl.when(valid(w) & here)
        def run():
            lax.fori_loop(0, lay.chips // wide, body, 0)

    for k in range(chunks):
        for w in reversed(early):
            pass_on(w, k)
        for i in lay.near:
            plane_wait(i, k)
        for i in lay.far:
            relay_copy(i, k).start()
        if C > 1:
            for i in lay.near:
                sibling_copy(i, k).start()

    def when_at(sixths):
        return min(chunks * sixths // 6, chunks - 1)

    plan = [[] for _ in range(chunks)]
    plan[when_at(0)].append(lambda: own_sweep("near"))
    for j, w in enumerate(reversed(early)):
        plan[when_at(1 + 2 * j)].append(lambda w=w: line_sweep(w, "near"))
        plan[when_at(2)].append(lambda w=w: line_sweep(w, "self"))
    plan[when_at(4)].append(lambda: own_sweep("far"))
    for j, w in enumerate(reversed(early)):
        plan[when_at(4 + j)].append(lambda w=w: line_sweep(w, "far"))
    split = n * 2 // 3 if chunks % 6 == 0 and n * 2 // 3 % GROUP == 0 else 0
    relaying = z == lay.top
    for w in late:
        if split:
            plan[(chunks * 2 + 2) // 3 - 1].append(
                lambda w=w: late_sweep(w, 0, split, jnp.logical_not(relaying))
            )
            plan[chunks - 1].append(lambda w=w: late_sweep(w, 0, n, relaying))
            plan[chunks - 1].append(
                lambda w=w: late_sweep(w, split, n - split, jnp.logical_not(relaying))
            )
        else:
            plan[chunks - 1].append(lambda w=w: late_sweep(w, 0, n, z >= 0))
    far_at = (chunks * 2 + 2) // 3 - 1
    far_pieces = [list(range(2 * k, min(2 * k + 2, chunks))) for k in range(chunks)]
    if chunks == 1:
        far_pieces = [[0]]
    for k in range(chunks):
        for w in late:
            pass_on(w, k)
        for j in far_pieces[k]:
            for i in lay.far:
                plane_wait(i, j)
                if C > 1:
                    sibling_copy(i, j).start()
        if C > 1 and k == 0:
            for i in lay.near:
                for j in range(chunks):
                    sibling_wait(i, j)
        if k == far_at:
            for i in lay.far:
                order_wait(i)
                if C > 1:
                    order_across(i, 0).start()
            if C > 1:
                for i in lay.far:
                    order_across(i, 1).wait_recv()
        if C > 1 and k == far_at:
            for i in lay.far:
                for j in range(chunks):
                    sibling_wait(i, j)
        for run in plan[k]:
            run()

    for one in range(lay.chips):
        flat = jnp.max(col_best[one], axis=0, keepdims=True)
        for core_at in range(C):
            plane_res[one * C + core_at] = flat[:, core_at * n:(core_at + 1) * n]

    for w in range(lay.top + 1):
        if w == 0 and not lay.down:
            continue

        def fold(w=w):
            line_res[w] = jnp.max(row_best[w].T, axis=0, keepdims=True)

        pl.when(valid(w))(fold)

    def result_copy(o):
        df, dx, dc = lay.peers[o]
        there = (lax.rem(f + df, F) * X + lax.rem(x + dx, X)) * C + lax.rem(core + dc, C)
        return remote(
            plane_res.at[there], plane_in.at[o], rs.at[o], rr.at[o], plane_id(df, dx, dc)
        )

    def line_result(w):
        there = z + 1 if w == 0 else base - w
        return remote(line_res.at[w], line_in.at[z], lrs.at[w], lrr.at[z], line_id(there))

    for w in range(lay.top + 1):
        if w == 0 and not lay.down:
            continue
        pl.when(valid(w))(lambda w=w: line_result(w).start())
    for o in range(len(lay.peers)):
        result_copy(o).start()

    best = jnp.maximum(plane_res[slot], jnp.float32(-1.0))
    for o in range(len(lay.peers)):
        result_copy(o).wait_recv()
        best = jnp.maximum(best, plane_in[o])
    line_best[...] = best.reshape(1, n)
    for src in range(S):
        def gather(src=src):
            remote(
                line_res.at[0], line_in.at[src], lrs.at[0], lrr.at[src], line_id(z)
            ).wait_recv()
            line_best[...] = jnp.maximum(line_best[...], line_in[src])

        pl.when(meets(z, jnp.int32(src)))(gather)

    out[...] = line_best[...].reshape(n)
    for k in range(chunks):
        pl.when(sends_up)(lambda k=k: line_copy(own_part(k), k, 1, lay.top + 1, z + 1).wait_send())
        if lay.down:
            pl.when(sends_down)(lambda k=k: line_copy(own_part(k), k, 0, 0, z - 1).wait_send())
        for i in lay.near:
            plane_copy(i, k).wait_send()
        for i in lay.far:
            relay_copy(i, k).wait_send()
        if C > 1:
            for i in range(-1, len(lay.offsets)):
                sibling_copy(i, k).wait_send()
        for w in range(1, lay.top + 1):
            for cond, copy in relays(w, k):
                pl.when(cond)(lambda copy=copy: copy.wait_send())
    for o in range(len(lay.peers)):
        result_copy(o).wait_send()
    for i in lay.near:
        order_copy(i).wait_send()
    for i in lay.far:
        order_relay(i).wait_send()
    if C > 1:
        for i in range(-1, len(lay.offsets)):
            order_across(i, 0).wait_send()
    pl.when(sends_up)(lambda: own_order(z + 1).wait_send())
    if lay.down:
        pl.when(sends_down)(lambda: own_order(z - 1).wait_send())
    for w in range(1, lay.top + 1):
        pl.when(goes_on(w))(lambda w=w: order_up(w).wait_send())
    for w in range(lay.top + 1):
        if w == 0 and not lay.down:
            continue
        pl.when(valid(w))(lambda w=w: line_result(w).wait_send())


def shards(lay, embeddings, doc_order):
    n, depth = embeddings.shape
    chunks = n // PIECE if n % PIECE == 0 else 1
    dma = pltpu.SemaphoreType.DMA
    near, peers, top, S = max(len(lay.offsets), 1), max(len(lay.peers), 1), lay.top, lay.slow
    found = pl.pallas_call(
        functools.partial(kernel, lay, n, chunks),
        out_shape=jax.ShapeDtypeStruct((n,), jnp.float32),
        in_specs=[pl.BlockSpec(memory_space=pltpu.VMEM)] * 2,
        out_specs=pl.BlockSpec(memory_space=pltpu.VMEM),
        scratch_shapes=[
            pltpu.VMEM((lay.plane * n, depth), jnp.bfloat16),
            pltpu.VMEM((top + 1, n, depth), jnp.bfloat16),
            pltpu.VMEM((lay.plane, 1, n), jnp.int32),
            pltpu.VMEM((S, 1, n), jnp.int32),
            pltpu.VMEM((top + 2, n, LANES), jnp.int32),
            pltpu.VMEM((top + 1, n, LANES), jnp.float32),
            pltpu.VMEM((lay.chips, 8, lay.cores * n), jnp.float32),
            pltpu.VMEM((lay.plane, 1, n), jnp.float32),
            pltpu.VMEM((top + 1, 1, n), jnp.float32),
            pltpu.VMEM((peers, 1, n), jnp.float32),
            pltpu.VMEM((S, 1, n), jnp.float32),
            pltpu.VMEM((1, n), jnp.float32),
            dma((near, chunks)), dma((near, chunks)),
            dma((near + 1, chunks)), dma((near + 1, chunks)),
            dma((top + 2, chunks)), dma((top + 1, chunks)),
            dma((near,)), dma((near,)),
            dma((top + 1,)), dma((S,)),
            dma((near + 1,)), dma((near + 1,)),
            dma((peers,)), dma((peers,)),
            dma((top + 1,)), dma((S,)),
        ],
        compiler_params=pltpu.CompilerParams(
            collective_id=0, has_side_effects=True, vmem_limit_bytes=60 * 1024 * 1024
        ),
    )(embeddings, doc_order)
    return found


def solution(mesh):
    lay = Layout(mesh.shape["row"], mesh.shape["col"])
    return jax.shard_map(
        functools.partial(shards, lay),
        mesh=mesh,
        in_specs=(P(("row", "col"), None), P(("row", "col"))),
        out_specs=P(("row", "col")),
        check_vma=False,
    )
```

```python
import functools

import jax
import jax.numpy as jnp
from jax import lax
from jax.experimental import pallas as pl
from jax.experimental.pallas import tpu as pltpu
from jax.sharding import PartitionSpec as P

MESH = pl.DeviceIdType.MESH
LANES = 128
PIECE = 64
GROUP = 128


def fast_size(rows):
    best = 1
    for size in range(1, rows + 1):
        if rows % size == 0 and size * size <= rows:
            best = size
    return best


class Layout:
    def __init__(self, rows, cols):
        self.fast = fast_size(rows)
        self.slow = rows // self.fast
        self.cores = 2 if cols % 2 == 0 else 1
        self.xs = cols // self.cores
        self.chips = self.fast * self.xs
        self.plane = self.chips * self.cores
        self.top = self.slow - 2 if self.slow > 2 else self.slow - 1
        self.down = self.slow > 2
        chips = [(f, x) for f in range(self.fast) for x in range(self.xs)]
        near = [c for c in chips if (c[0] == 0) != (c[1] == 0)]
        far = [c for c in chips if c[0] != 0 and c[1] != 0]
        self.offsets = near + far
        self.near = list(range(len(near)))
        self.far = list(range(len(near), len(near) + len(far)))
        self.peers = [
            (f, x, c)
            for f in range(self.fast)
            for x in range(self.xs)
            for c in range(self.cores)
            if (f, x, c) != (0, 0, 0)
        ]


def kernel(
    lay, n, chunks,
    emb, order, out,
    units, line, orders, line_orders, col_orders,
    row_best, col_best, plane_res, line_res, plane_in, line_in, line_best,
    ps, pr, ss, sr, ls, lr, os_, or_, los, lor, oss, osr, rs, rr, lrs, lrr,
):
    S, F, X, C = lay.slow, lay.fast, lay.xs, lay.cores
    rows_here = n // chunks
    align = PIECE if rows_here % PIECE == 0 else rows_here
    r, c = lax.axis_index("row"), lax.axis_index("col")
    z, f = r // F, lax.rem(r, F)
    x, core = c // C, lax.rem(c, C)
    chip = f * X + x
    slot = chip * C + core

    def plane_id(df, dx, dc):
        return {
            "row": z * F + lax.rem(f + df, F),
            "col": lax.rem(x + dx, X) * C + lax.rem(core + dc, C),
        }

    def line_id(there):
        return {"row": there * F + f, "col": c}

    def source_chip(df, dx):
        return lax.rem(f + F - df, F) * X + lax.rem(x + X - dx, X)

    def span(which, k):
        return pl.ds(pl.multiple_of(which * n + k * rows_here, align), rows_here)

    def remote(src, dst, send, recv, where):
        return pltpu.make_async_remote_copy(
            src_ref=src, dst_ref=dst, send_sem=send, recv_sem=recv,
            device_id=where, device_id_type=MESH,
        )

    def plane_copy(i, k):
        part = units.at[span(slot, k)]
        return remote(part, part, ps.at[i, k], pr.at[i, k], plane_id(*lay.offsets[i], 0))

    def relay_copy(i, k):
        df, dx = lay.offsets[i]
        src, step = ((0, dx), (df, 0)) if k % 2 == 0 else ((df, 0), (0, dx))
        part = units.at[span(source_chip(*src) * C + core, k)]
        return remote(part, part, ps.at[i, k], pr.at[i, k], plane_id(*step, 0))

    def sibling_copy(i, k):
        src = chip if i < 0 else source_chip(*lay.offsets[i])
        part = units.at[span(src * C + core, k)]
        return remote(part, part, ss.at[i + 1, k], sr.at[i + 1, k], plane_id(0, 0, 1))

    def plane_wait(i, k):
        src = source_chip(*lay.offsets[i]) * C + core
        part = units.at[span(src, k)]
        remote(part, part, ps.at[i, k], pr.at[i, k], plane_id(*lay.offsets[i], 0)).wait_recv()

    def sibling_wait(i, k):
        src = chip if i < 0 else source_chip(*lay.offsets[i])
        part = units.at[span(src * C + lax.rem(core + 1, C), k)]
        remote(part, part, ss.at[i + 1, k], sr.at[i + 1, k], plane_id(0, 0, 1)).wait_recv()

    def line_copy(src, k, dst_slot, tag, there):
        return remote(
            src, line.at[dst_slot, pl.ds(k * rows_here, rows_here)],
            ls.at[tag, k], lr.at[dst_slot, k], line_id(there),
        )

    def own_part(k):
        return units.at[span(slot, k)]

    base = jnp.minimum(z, lay.top)
    sends_up = z < lay.top
    last = S - 1
    sends_down = (z == last) if lay.down else None
    takes_down = (z == last - 1) if lay.down else None

    def relays(w, k):
        part = line.at[w, pl.ds(k * rows_here, rows_here)]
        found = []
        if w < lay.top:
            found.append(((base >= w) & (z < lay.top), line_copy(part, k, w + 1, w, z + 1)))
        if lay.down:
            found.append(((base >= w) & (z == lay.top), line_copy(part, k, w, w, z + 1)))
        return found

    def order_send(src, i, where):
        return remote(orders.at[src], orders.at[src], os_.at[i], or_.at[i], where)

    def order_copy(i):
        return order_send(slot, i, plane_id(*lay.offsets[i], 0))

    def order_relay(i):
        df, dx = lay.offsets[i]
        return order_send(source_chip(0, dx) * C + core, i, plane_id(df, 0, 0))

    def order_wait(i):
        order_send(source_chip(*lay.offsets[i]) * C + core, i, plane_id(0, 0, 1)).wait_recv()

    def order_across(i, side):
        src = chip if i < 0 else source_chip(*lay.offsets[i])
        part = orders.at[src * C + lax.rem(core + side, C)]
        return remote(part, part, oss.at[i + 1], osr.at[i + 1], plane_id(0, 0, 1))

    def meets(src, dst):
        up = (src < dst) & ((src != lay.top) | (not lay.down))
        if lay.down:
            up = up | ((src == last) & (dst == last - 1))
        return up

    def line_order_copy(part, src, tag, there):
        return remote(part, line_orders.at[src], los.at[tag], lor.at[src], line_id(there))

    def own_order(there):
        return line_order_copy(orders.at[slot], z, 0, there)

    def order_up(w):
        return line_order_copy(line_orders.at[base - w], base - w, w, z + 1)

    def goes_on(w):
        return (base >= w) & (z < last) & (lay.down | (z < lay.top))

    barrier = pltpu.get_barrier_semaphore()
    steps = [(*lay.offsets[i], 0) for i in lay.near] + ([(0, 0, 1)] if C > 1 else [])
    sides = ((z > 0, z - 1), (z < last, z + 1))
    for step in steps:
        pl.semaphore_signal(barrier, inc=1, device_id=plane_id(*step), device_id_type=MESH)
    for there, which in sides:
        pl.when(there)(
            lambda which=which: pl.semaphore_signal(
                barrier, inc=1, device_id=line_id(which), device_id_type=MESH
            )
        )

    orders[pl.ds(slot, 1)] = order[...].reshape(1, 1, n)

    def spread(which, row):
        wide = jnp.broadcast_to(row.reshape(1, n), (LANES, n))
        col_orders[which] = wide.T

    def normalize(k):
        floats = emb[pl.ds(k * rows_here, rows_here), :].astype(jnp.float32)
        scale = lax.rsqrt(jnp.sum(floats * floats, axis=1, keepdims=True) + 1e-06)
        units[span(slot, k), :] = (floats * scale).astype(jnp.bfloat16)

    def send_own(k):
        pl.when(sends_up)(lambda: line_copy(own_part(k), k, 1, lay.top + 1, z + 1).start())
        if lay.down:
            pl.when(sends_down)(lambda: line_copy(own_part(k), k, 0, 0, z - 1).start())
        for i in lay.near:
            plane_copy(i, k).start()
        if C > 1:
            sibling_copy(-1, k).start()

    for k in range(chunks):
        normalize(k)
    lines = jnp.minimum(z, 1) + jnp.minimum(last - z, 1)
    pl.semaphore_wait(barrier, len(steps) + lines)
    pl.when(sends_up)(lambda: own_order(z + 1).start())
    if lay.down:
        pl.when(sends_down)(lambda: own_order(z - 1).start())
    for i in lay.near:
        order_copy(i).start()
    if C > 1:
        order_across(-1, 0).start()
    for k in range(chunks):
        send_own(k)

    row_best[...] = jnp.full(row_best.shape, -1.0, jnp.float32)
    col_best[...] = jnp.full(col_best.shape, -1.0, jnp.float32)
    spread(lay.top + 1, order[...].reshape(1, n))

    width = C * n

    def item(lhs, w, first_chip, both, first=0, count=n, wide=1):
        rhs = units[pl.ds(pl.multiple_of(first_chip * width, LANES), wide * width), :]
        s = lax.dot_general(
            lhs, rhs, (((1,), (1,)), ((), ())), preferred_element_type=jnp.float32
        )
        mine = col_orders[w, first:first + count, :]
        rows_max = None
        for j in range(wide * width // LANES):
            part = s[:, j * LANES:(j + 1) * LANES]
            which_chip, at = first_chip + j * LANES // width, j * LANES % width
            core_at, lane_at = at // n, at % n
            theirs = orders[which_chip * C + core_at, :, lane_at:lane_at + LANES]
            earlier = theirs < mine
            if both:
                cand = jnp.where(earlier, part, jnp.float32(-1.0))
                rows_max = cand if rows_max is None else jnp.maximum(rows_max, cand)
                later = jnp.where(earlier, jnp.float32(-1.0), part)
            else:
                later = jnp.where(mine < theirs, part, jnp.float32(-1.0))
            down = jnp.max(later.reshape(count // 8, 8, LANES), axis=0)
            col_best[which_chip, :, at:at + LANES] = jnp.maximum(
                col_best[which_chip, :, at:at + LANES], down
            )
        if both:
            row_best[w, first:first + count, :] = jnp.maximum(
                row_best[w, first:first + count, :], rows_max
            )

    def own_item(which_chip):
        lhs = units[pl.ds(pl.multiple_of(slot * n, LANES), n), :]
        item(lhs, lay.top + 1, which_chip, False)

    def line_item(w, which_chip):
        item(line[w], w, which_chip, True)

    def valid(w):
        return takes_down if w == 0 else base >= w

    early = [w for w in ([0] if lay.down else []) + [1] if w <= lay.top]
    late = list(range(2, lay.top + 1))

    def take_order(w):
        src = (z + 1) if w == 0 else base - w
        line_order_copy(line_orders.at[src], src, 0, z).wait_recv()
        if w > 0:
            pl.when(goes_on(w))(lambda: order_up(w).start())
        spread(w, line_orders[src])

    for i in lay.near:
        order_wait(i)
        if C > 1:
            order_across(i, 0).start()
    for i in lay.far:
        order_relay(i).start()
    if C > 1:
        order_across(-1, 1).wait_recv()
        for k in range(chunks):
            sibling_wait(-1, k)
    own_item(chip)
    if C > 1:
        for i in lay.near:
            order_across(i, 1).wait_recv()

    def line_wait(w, k):
        line_copy(line.at[w, pl.ds(k * rows_here, rows_here)], k, w, 0, z).wait_recv()

    def pass_on(w, k):
        if k == 0:
            pl.when(valid(w))(lambda: take_order(w))
        pl.when(valid(w))(lambda: line_wait(w, k))
        if w > 0:
            for cond, copy in relays(w, k):
                pl.when(cond)(lambda copy=copy: copy.start())

    def chips_of(places):
        def at(j):
            if places == "near":
                by_x = j < X - 1
                df = jnp.where(by_x, 0, j - (X - 2))
                dx = jnp.where(by_x, j + 1, 0)
            elif places == "far":
                df, dx = 1 + j // max(X - 1, 1), 1 + lax.rem(j, max(X - 1, 1))
            elif places == "self":
                df, dx = 0, 0
            else:
                df, dx = j // X, lax.rem(j, X)
            return source_chip(df, dx)

        count = {"near": F + X - 2, "far": (F - 1) * (X - 1), "self": 1, "all": F * X}
        return count[places], at

    def loop(places, body):
        count, at = chips_of(places)

        def step(j, carry):
            body(at(j))
            return carry

        if count:
            lax.fori_loop(0, count, step, 0)

    def own_sweep(places):
        loop(places, own_item)

    def line_sweep(w, places):
        pl.when(valid(w))(lambda: loop(places, lambda one: line_item(w, one)))

    wide = next(m for m in (4, 3, 2, 1) if lay.chips % m == 0)

    def late_sweep(w, first, count, here):
        def body(j, carry):
            item(line[w, first:first + count, :], w, j * wide, True, first, count, wide)
            return carry

        @pl.when(valid(w) & here)
        def run():
            lax.fori_loop(0, lay.chips // wide, body, 0)

    for k in range(chunks):
        for w in reversed(early):
            pass_on(w, k)
        for i in lay.near:
            plane_wait(i, k)
        for i in lay.far:
            relay_copy(i, k).start()
        if C > 1:
            for i in lay.near:
                sibling_copy(i, k).start()

    def line_result(w):
        there = z + 1 if w == 0 else base - w
        return remote(line_res.at[w], line_in.at[z], lrs.at[w], lrr.at[z], line_id(there))

    def give_back(w):
        @pl.when(valid(w))
        def fold():
            line_res[w] = jnp.max(row_best[w].T, axis=0, keepdims=True)
            line_result(w).start()

    def when_at(sixths):
        return min(chunks * sixths // 6, chunks - 1)

    plan = [[] for _ in range(chunks)]
    plan[when_at(0)].append(lambda: own_sweep("near"))
    for j, w in enumerate(reversed(early)):
        plan[when_at(1 + 2 * j)].append(lambda w=w: line_sweep(w, "near"))
        plan[when_at(2)].append(lambda w=w: line_sweep(w, "self"))
    plan[when_at(4)].append(lambda: own_sweep("far"))
    for j, w in enumerate(reversed(early)):
        plan[when_at(4 + j)].append(lambda w=w: line_sweep(w, "far"))
    split = n * 2 // 3 if chunks % 6 == 0 and n * 2 // 3 % GROUP == 0 else 0
    relaying = z == lay.top
    for w in reversed(early):
        plan[chunks - 1].append(lambda w=w: give_back(w))
    for w in late:
        if split:
            plan[(chunks * 2 + 2) // 3 - 1].append(
                lambda w=w: late_sweep(w, 0, split, jnp.logical_not(relaying))
            )
            plan[chunks - 1].append(lambda w=w: late_sweep(w, 0, n, relaying))
            plan[chunks - 1].append(
                lambda w=w: late_sweep(w, split, n - split, jnp.logical_not(relaying))
            )
        else:
            plan[chunks - 1].append(lambda w=w: late_sweep(w, 0, n, z >= 0))
    far_at = (chunks * 2 + 2) // 3 - 1
    far_pieces = [list(range(2 * k, min(2 * k + 2, chunks))) for k in range(chunks)]
    if chunks == 1:
        far_pieces = [[0]]
    for k in range(chunks):
        for w in late:
            pass_on(w, k)
        for j in far_pieces[k]:
            for i in lay.far:
                plane_wait(i, j)
                if C > 1:
                    sibling_copy(i, j).start()
        if C > 1 and k == 0:
            for i in lay.near:
                for j in range(chunks):
                    sibling_wait(i, j)
        if k == far_at:
            for i in lay.far:
                order_wait(i)
                if C > 1:
                    order_across(i, 0).start()
            if C > 1:
                for i in lay.far:
                    order_across(i, 1).wait_recv()
        if C > 1 and k == far_at:
            for i in lay.far:
                for j in range(chunks):
                    sibling_wait(i, j)
        for run in plan[k]:
            run()

    for w in late:
        give_back(w)

    for one in range(lay.chips):
        flat = jnp.max(col_best[one], axis=0, keepdims=True)
        for core_at in range(C):
            plane_res[one * C + core_at] = flat[:, core_at * n:(core_at + 1) * n]

    def result_copy(o):
        df, dx, dc = lay.peers[o]
        there = (lax.rem(f + df, F) * X + lax.rem(x + dx, X)) * C + lax.rem(core + dc, C)
        return remote(
            plane_res.at[there], plane_in.at[o], rs.at[o], rr.at[o], plane_id(df, dx, dc)
        )

    for o in range(len(lay.peers)):
        result_copy(o).start()

    best = jnp.maximum(plane_res[slot], jnp.float32(-1.0))
    for o in range(len(lay.peers)):
        result_copy(o).wait_recv()
        best = jnp.maximum(best, plane_in[o])
    line_best[...] = best.reshape(1, n)
    for src in range(S):
        def gather(src=src):
            remote(
                line_res.at[0], line_in.at[src], lrs.at[0], lrr.at[src], line_id(z)
            ).wait_recv()
            line_best[...] = jnp.maximum(line_best[...], line_in[src])

        pl.when(meets(z, jnp.int32(src)))(gather)

    out[...] = line_best[...].reshape(n)
    for k in range(chunks):
        pl.when(sends_up)(lambda k=k: line_copy(own_part(k), k, 1, lay.top + 1, z + 1).wait_send())
        if lay.down:
            pl.when(sends_down)(lambda k=k: line_copy(own_part(k), k, 0, 0, z - 1).wait_send())
        for i in lay.near:
            plane_copy(i, k).wait_send()
        for i in lay.far:
            relay_copy(i, k).wait_send()
        if C > 1:
            for i in range(-1, len(lay.offsets)):
                sibling_copy(i, k).wait_send()
        for w in range(1, lay.top + 1):
            for cond, copy in relays(w, k):
                pl.when(cond)(lambda copy=copy: copy.wait_send())
    for o in range(len(lay.peers)):
        result_copy(o).wait_send()
    for i in lay.near:
        order_copy(i).wait_send()
    for i in lay.far:
        order_relay(i).wait_send()
    if C > 1:
        for i in range(-1, len(lay.offsets)):
            order_across(i, 0).wait_send()
    pl.when(sends_up)(lambda: own_order(z + 1).wait_send())
    if lay.down:
        pl.when(sends_down)(lambda: own_order(z - 1).wait_send())
    for w in range(1, lay.top + 1):
        pl.when(goes_on(w))(lambda w=w: order_up(w).wait_send())
    for w in range(lay.top + 1):
        if w == 0 and not lay.down:
            continue
        pl.when(valid(w))(lambda w=w: line_result(w).wait_send())


def shards(lay, embeddings, doc_order):
    n, depth = embeddings.shape
    chunks = n // PIECE if n % PIECE == 0 else 1
    dma = pltpu.SemaphoreType.DMA
    near, peers, top, S = max(len(lay.offsets), 1), max(len(lay.peers), 1), lay.top, lay.slow
    found = pl.pallas_call(
        functools.partial(kernel, lay, n, chunks),
        out_shape=jax.ShapeDtypeStruct((n,), jnp.float32),
        in_specs=[pl.BlockSpec(memory_space=pltpu.VMEM)] * 2,
        out_specs=pl.BlockSpec(memory_space=pltpu.VMEM),
        scratch_shapes=[
            pltpu.VMEM((lay.plane * n, depth), jnp.bfloat16),
            pltpu.VMEM((top + 1, n, depth), jnp.bfloat16),
            pltpu.VMEM((lay.plane, 1, n), jnp.int32),
            pltpu.VMEM((S, 1, n), jnp.int32),
            pltpu.VMEM((top + 2, n, LANES), jnp.int32),
            pltpu.VMEM((top + 1, n, LANES), jnp.float32),
            pltpu.VMEM((lay.chips, 8, lay.cores * n), jnp.float32),
            pltpu.VMEM((lay.plane, 1, n), jnp.float32),
            pltpu.VMEM((top + 1, 1, n), jnp.float32),
            pltpu.VMEM((peers, 1, n), jnp.float32),
            pltpu.VMEM((S, 1, n), jnp.float32),
            pltpu.VMEM((1, n), jnp.float32),
            dma((near, chunks)), dma((near, chunks)),
            dma((near + 1, chunks)), dma((near + 1, chunks)),
            dma((top + 2, chunks)), dma((top + 1, chunks)),
            dma((near,)), dma((near,)),
            dma((top + 1,)), dma((S,)),
            dma((near + 1,)), dma((near + 1,)),
            dma((peers,)), dma((peers,)),
            dma((top + 1,)), dma((S,)),
        ],
        compiler_params=pltpu.CompilerParams(
            collective_id=0, has_side_effects=True, vmem_limit_bytes=60 * 1024 * 1024
        ),
    )(embeddings, doc_order)
    return found


def solution(mesh):
    lay = Layout(mesh.shape["row"], mesh.shape["col"])
    return jax.shard_map(
        functools.partial(shards, lay),
        mesh=mesh,
        in_specs=(P(("row", "col"), None), P(("row", "col"))),
        out_specs=P(("row", "col")),
        check_vma=False,
    )
```
